32 devices in a mesh: outer: 4 (over z), inner: 8 (over y, x, core).
Axes of the slice: x: 2, y: 2, z: 4, core: 2. Of those that a mesh axis runs over, the one named last changes fastest.
Arguments:
- query_gate: bfloat16 [4096, 4096], P(None, ('outer', 'inner')), may hold values from -6 to 6
- key_proj: bfloat16 [4096, 4096], P(None, ('outer', 'inner')), may hold values from -6 to 6
- value_proj: bfloat16 [4096, 4096], P(None, ('outer', 'inner')), may hold values from -6 to 6
- out_grad: bfloat16 [4096, 4096], P(None, ('outer', 'inner')), may hold values from -6 to 6
- filters: float32 [4096, 4096], P(None, ('outer', 'inner')), may hold values from -8 to 8
- skip_bias: float32 [4096], P(('outer', 'inner')), may hold values from -4 to 4
Outputs:
- output: bfloat16 [4096, 4096], P(None, ('outer', 'inner'))
- query_grad: bfloat16 [4096, 4096], P(None, ('outer', 'inner'))
- key_grad: bfloat16 [4096, 4096], P(None, ('outer', 'inner'))
- value_grad: bfloat16 [4096, 4096], P(None, ('outer', 'inner'))
- filter_grad: float32 [4096, 4096], P(None, ('outer', 'inner'))
- bias_grad: float32 [4096], P(('outer', 'inner'))
The draws below stay inside these ranges and needn't reach their ends.
All inputs are finite; a program needn't handle non-finite values.
Results may differ from the reference program's by a relative error of at most 0.0058.
Values may be sent and summed in bfloat16 or wider, within the bound.
A program may use at most 128 MiB of HBM per device.

```python
import math
import jax
import jax.numpy as jnp
from jax import lax

D = 4096
SEQUENCE_LENGTH = 4096


def draw_filters(key, part):
    jitter_random_key, variety_random_key, quick_random_key, gradual_random_key, spike_random_key, scale_random_key = jax.random.split(key, 6)
    noise_vals = jnp.clip(jax.random.normal(jitter_random_key, (D, SEQUENCE_LENGTH), jnp.float32), -4.0, 4.0)
    kind_draw = jax.random.randint(variety_random_key, (D, 1), 0, 10)
    position_index = jnp.arange(SEQUENCE_LENGTH, dtype=jnp.float32)[None, :]
    fast_decay = jnp.exp(jax.random.uniform(quick_random_key, (D, 1), jnp.float32, math.log(10.0), math.log(20.0)))
    slow_decay = jnp.exp(jax.random.uniform(gradual_random_key, (D, 1), jnp.float32, math.log(2.0 * SEQUENCE_LENGTH), math.log(8.0 * SEQUENCE_LENGTH)))
    spike_position = jax.random.randint(spike_random_key, (3,), 0, SEQUENCE_LENGTH).astype(jnp.float32)
    spike_factor = jnp.prod(jnp.where(position_index[:, :, None] >= spike_position[None, None, :], 0.7, 1.0), axis=-1)
    slow_mask = kind_draw >= 5
    chan_scale = jnp.exp(jax.random.uniform(scale_random_key, (D, 1), jnp.float32, math.log(0.5), math.log(2.0)))
    decay_length = jnp.where(slow_mask, slow_decay, fast_decay)
    decay_profile = jnp.exp(-position_index / decay_length) * spike_factor
    norm_factor = jnp.sqrt(2.0 / jnp.minimum(decay_length, float(SEQUENCE_LENGTH)))
    return noise_vals * decay_profile * norm_factor * chan_scale


def shard_levels(own_key, extent, pieces, least, top_value):
    gain, own = 1.0, jax.random.fold_in(own_key, 6)
    for axis_at, parts in pieces:
        steps = jnp.exp(jax.random.uniform(jax.random.fold_in(own, axis_at), (parts,), jnp.float32, least / len(pieces), top_value / len(pieces)))
        gain = gain * jnp.repeat(steps, extent[axis_at] // parts).reshape([-1 if axis == axis_at else 1 for axis in range(len(extent))])
    return gain


def bell_draw(own_key, shape, spread, reach, cuts=(), held_as=jnp.bfloat16):
    values = spread * jax.random.normal(own_key, shape, jnp.float32)
    if cuts:
        values = values * shard_levels(own_key, shape, cuts, -0.22, 0.18)
    return jnp.clip(values, -reach, reach).astype(held_as)


def setup_inputs(seed: int = 0) -> dict:
    arg_keys = jax.random.split(jax.random.key(seed), 7)
    query_gate = bell_draw(arg_keys[0], (D, SEQUENCE_LENGTH), 1.0, 6.0, ((1, 32),))
    key_proj = bell_draw(arg_keys[1], (D, SEQUENCE_LENGTH), 1.0, 6.0, ((1, 32),))
    value_proj = bell_draw(arg_keys[2], (D, SEQUENCE_LENGTH), 1.0, 6.0, ((1, 32),))
    out_grad = bell_draw(arg_keys[3], (D, SEQUENCE_LENGTH), 1.0, 6.0, ((1, 32),))
    filters = draw_filters(jax.random.fold_in(arg_keys[6], 71), 0)
    skip_bias = bell_draw(arg_keys[5], (D,), 1.0, 4.0, ((0, 32),), jnp.float32)
    return dict(query_gate=query_gate, key_proj=key_proj, value_proj=value_proj, out_grad=out_grad, filters=filters, skip_bias=skip_bias)


def channel_block(inputs):
    mixed_blk, filter_blk, query_blk, grad_blk, key_blk, value_blk, bias_blk = inputs
    total = 2 * SEQUENCE_LENGTH
    mixed_wide = mixed_blk.astype(jnp.float32)
    mixed_spec = jnp.fft.rfft(mixed_wide, n=total, axis=-1)
    filter_spec = jnp.fft.rfft(filter_blk, n=total, axis=-1)
    conv_rows = jnp.fft.irfft(mixed_spec * filter_spec, n=total, axis=-1)[:, :SEQUENCE_LENGTH]
    bias_col = bias_blk[:, None]
    convolved = (conv_rows + bias_col * mixed_wide).astype(jnp.bfloat16)
    conv_wide = convolved.astype(jnp.float32)
    query_wide = query_blk.astype(jnp.float32)
    grad_wide = grad_blk.astype(jnp.float32)
    output = (query_wide * conv_wide).astype(jnp.bfloat16)
    query_grad = (grad_wide * conv_wide).astype(jnp.bfloat16)
    gated = (grad_wide * query_wide).astype(jnp.bfloat16)
    gated_wide = gated.astype(jnp.float32)
    gated_spec = jnp.fft.rfft(gated_wide, n=total, axis=-1)
    back_rows = jnp.fft.irfft(gated_spec * jnp.conj(filter_spec), n=total, axis=-1)[:, :SEQUENCE_LENGTH]
    mixed_grad = (back_rows + bias_col * gated_wide).astype(jnp.bfloat16)
    grad_wide_mix = mixed_grad.astype(jnp.float32)
    key_grad = (grad_wide_mix * value_blk.astype(jnp.float32)).astype(jnp.bfloat16)
    value_grad = (grad_wide_mix * key_blk.astype(jnp.float32)).astype(jnp.bfloat16)
    grad_scale = 1.0 / math.sqrt(SEQUENCE_LENGTH)
    filter_grad = jnp.fft.irfft(gated_spec * jnp.conj(mixed_spec), n=total, axis=-1)[:, :SEQUENCE_LENGTH] * grad_scale
    bias_grad = lax.optimization_barrier(jnp.sum(gated_wide * mixed_wide, axis=1)) * grad_scale
    return (output, query_grad, key_grad, value_grad, filter_grad, bias_grad)

def reference(query_gate, key_proj, value_proj, out_grad, filters, skip_bias):
    mixed = (key_proj.astype(jnp.float32) * value_proj.astype(jnp.float32)).astype(jnp.bfloat16)
    groups = D // 128

    def split_rows(array):
        return array.reshape(groups, 128, SEQUENCE_LENGTH)
    stacked = (split_rows(mixed), split_rows(filters), split_rows(query_gate), split_rows(out_grad), split_rows(key_proj), split_rows(value_proj), skip_bias.reshape(groups, 128))
    output, query_grad, key_grad, value_grad, filter_grad, bias_grad = lax.map(channel_block, stacked)
    return (output.reshape(D, SEQUENCE_LENGTH), query_grad.reshape(D, SEQUENCE_LENGTH), key_grad.reshape(D, SEQUENCE_LENGTH), value_grad.reshape(D, SEQUENCE_LENGTH), filter_grad.reshape(D, SEQUENCE_LENGTH), bias_grad.reshape(D))
```

```python
import math

import jax
import jax.numpy as jnp
import numpy as np
from jax import lax
from jax.sharding import PartitionSpec as P

AXES = ("outer", "inner")
PREC = lax.Precision.HIGH


def tables(blocks, fine):
    total = 2 * blocks * fine
    a = np.arange(blocks)
    p = np.arange(blocks)
    r = np.arange(fine)
    coarse = 2.0 * math.pi * ((2 * a[:, None] + 1) * p[None, :] % (4 * blocks)) / (4 * blocks)
    twist = 2.0 * math.pi * ((2 * a[:, None] + 1) * r[None, :]) / (2 * total)
    inner = 2.0 * math.pi * (r[:, None] * r[None, :] % fine) / fine
    cos_f, sin_f = np.cos(inner), np.sin(inner)
    first = np.concatenate([np.cos(coarse), -np.sin(coarse)], 0)
    second = np.block([[cos_f, -sin_f], [sin_f, cos_f]])
    f32 = lambda x: jnp.asarray(x.astype(np.float32))
    return (
        f32(first),
        f32(np.cos(twist))[:, None, :],
        f32(np.sin(twist))[:, None, :],
        f32(second),
        f32(second.T),
        f32(first.T * (2.0 / total)),
    )


def forward(x, tabs):
    first, cos_t, sin_t, second, _, _ = tabs
    n, _, fine = x.shape
    z = jnp.einsum("ap,pcr->acr", first, x.astype(jnp.float32), precision=PREC)
    re, im = z[:n], z[n:]
    t = jnp.concatenate([re * cos_t + im * sin_t, im * cos_t - re * sin_t], axis=-1)
    s = jnp.einsum("acr,rb->acb", t, second, precision=PREC)
    return s[..., :fine], s[..., fine:]


def inverse(spec, tabs):
    _, cos_t, sin_t, _, second, last = tabs
    fine = spec[0].shape[-1]
    mid = jnp.einsum("acr,rb->acb", jnp.concatenate(spec, axis=-1), second, precision=PREC)
    re, im = mid[..., :fine], mid[..., fine:]
    t = jnp.concatenate([re * cos_t - im * sin_t, im * cos_t + re * sin_t], axis=0)
    return jnp.einsum("pa,acr->pcr", last, t, precision=PREC)


def multiply(left, right, conjugate):
    a, b = left
    c, d = right
    if conjugate:
        return (a * c + b * d, b * c - a * d)
    return (a * c - b * d, a * d + b * c)


def exchange(x):
    return lax.all_to_all(x, AXES, split_axis=0, concat_axis=0, tiled=True)


def make(n):
    def on_device(query_gate, key_proj, value_proj, out_grad, filters, skip_bias):
        f32, bf16 = jnp.float32, jnp.bfloat16
        total_channels, fine = key_proj.shape
        channels = total_channels // n
        length = n * fine
        tabs = tables(n, fine)
        shape = (n, channels, fine)

        gated_seq = (out_grad.astype(f32) * query_gate.astype(f32)).astype(bf16)
        mixed_seq = (key_proj.astype(f32) * value_proj.astype(f32)).astype(bf16)
        filter_seq = filters.astype(bf16)

        gated = exchange(gated_seq).reshape(shape)
        mixed_seq, gated = lax.optimization_barrier((mixed_seq, gated))
        mixed = exchange(mixed_seq).reshape(shape)
        filter_seq, mixed = lax.optimization_barrier((filter_seq, mixed))
        filt = exchange(filter_seq).reshape(shape)

        scale = 1.0 / math.sqrt(length)
        gated_spec = forward(gated, tabs)
        mixed_spec = forward(mixed, tabs)
        fg = (inverse(multiply(gated_spec, mixed_spec, True), tabs) * scale).astype(bf16)
        gated_wide = gated.astype(f32)
        mixed_wide = mixed.astype(f32)
        bias_grad = jnp.sum(gated_wide * mixed_wide, axis=(0, 2)) * scale
        fg, filt = lax.optimization_barrier((fg, filt))
        fg_seq = exchange(fg.reshape(total_channels, fine))

        filter_spec = forward(filt, tabs)
        bias = skip_bias[None, :, None]
        conv = inverse(multiply(filter_spec, mixed_spec, False), tabs)
        convolved = (conv + bias * mixed_wide).astype(bf16)
        convolved, fg_seq = lax.optimization_barrier((convolved, fg_seq))
        conv_seq = exchange(convolved.reshape(total_channels, fine))
        back = inverse(multiply(gated_spec, filter_spec, True), tabs)
        mixed_grad = (back + bias * gated_wide).astype(bf16)
        mixed_grad, conv_seq = lax.optimization_barrier((mixed_grad, conv_seq))
        grad_seq = exchange(mixed_grad.reshape(total_channels, fine))

        conv_wide = conv_seq.astype(f32)
        output = (query_gate.astype(f32) * conv_wide).astype(bf16)
        query_grad = (out_grad.astype(f32) * conv_wide).astype(bf16)
        grad_wide = grad_seq.astype(f32)
        key_grad = (grad_wide * value_proj.astype(f32)).astype(bf16)
        value_grad = (grad_wide * key_proj.astype(f32)).astype(bf16)
        return (output, query_grad, key_grad, value_grad, fg_seq.astype(f32), bias_grad)

    return on_device


def solution(mesh):
    n = math.prod(mesh.shape[a] for a in AXES)
    seq = P(None, AXES)
    return jax.shard_map(
        make(n),
        mesh=mesh,
        in_specs=(seq, seq, seq, seq, seq, P(AXES)),
        out_specs=(seq, seq, seq, seq, seq, P(AXES)),
        check_vma=False,
    )
```

```python
import functools
import math

import jax
import jax.numpy as jnp
import numpy as np
from jax import lax
from jax.experimental import pallas as pl
from jax.experimental.pallas import tpu as pltpu
from jax.sharding import PartitionSpec as P

AXES = ("outer", "inner")
MESH = pl.DeviceIdType.MESH
F32, BF16 = jnp.float32, jnp.bfloat16


def tables(blocks, fine):
    total = 2 * blocks * fine
    a = np.arange(blocks)
    p = np.arange(blocks)
    r = np.arange(fine)
    coarse = 2.0 * math.pi * ((2 * a[:, None] + 1) * p[None, :] % (4 * blocks)) / (4 * blocks)
    twist = 2.0 * math.pi * ((2 * a[:, None] + 1) * r[None, :]) / (2 * total)
    inner = 2.0 * math.pi * (r[:, None] * r[None, :] % fine) / fine
    cos_f, sin_f = np.cos(inner), np.sin(inner)
    first = np.concatenate([np.cos(coarse), -np.sin(coarse)], 0)
    second = np.block([[cos_f, -sin_f], [sin_f, cos_f]])
    last = first.T * (2.0 / total)

    def split(x):
        hi = x.astype(np.float32).astype(jnp.bfloat16)
        lo = (x - hi.astype(np.float64)).astype(np.float32).astype(jnp.bfloat16)
        return hi, lo

    first_hi, first_lo = split(first)
    return (
        np.concatenate([first_hi, first_lo], 0),
        np.cos(twist).astype(np.float32),
        np.sin(twist).astype(np.float32),
        np.stack(split(second)),
        np.stack(split(np.ascontiguousarray(second.T))),
        np.stack(split(last)),
    )


def halves(x):
    hi = x.astype(BF16)
    return hi, (x - hi.astype(F32)).astype(BF16)


def dot(a, b):
    return jnp.dot(a, b, preferred_element_type=F32)


def kernel(
    n, inner_size, scale,
    g_in, m_in, h_in, bias_ref, first_ref, cos_ref, sin_ref, second_ref, back_ref, last_ref,
    fg_out, conv_out, grad_out, dot_out,
    g_rows, m_rows, h_rows, fg_send, conv_send, grad_send, wide, result, g_spec, m_spec, h_spec,
    send_sem, recv_sem, own_sem,
):
    me = lax.axis_index("outer") * inner_size + lax.axis_index("inner")
    channels, fine = bias_ref.shape
    group = max(1, 256 // n)
    steps = channels // group

    def device(peer):
        return (peer // inner_size, peer % inner_size)

    barrier = pltpu.get_barrier_semaphore()

    @pl.loop(1, n)
    def _(d):
        peer = (me + d) % n
        pl.semaphore_signal(barrier, inc=1, device_id=device(peer), device_id_type=MESH)

    pl.semaphore_wait(barrier, n - 1)

    def remote(src, dst, phase, d):
        to = (me + d) % n
        return pltpu.make_async_remote_copy(
            src_ref=src.at[to],
            dst_ref=dst.at[me],
            send_sem=send_sem.at[phase, d],
            recv_sem=recv_sem.at[phase, d],
            device_id=device(to),
            device_id_type=MESH,
        )

    def arrival(src, dst, phase, d):
        come = (me + n - d) % n
        return pltpu.make_async_remote_copy(
            src_ref=src.at[come],
            dst_ref=dst.at[come],
            send_sem=send_sem.at[phase, d],
            recv_sem=recv_sem.at[phase, d],
            device_id=device(come),
            device_id_type=MESH,
        )

    def start(src, dst, phase):
        pltpu.make_async_copy(src.at[me], dst.at[me], own_sem.at[phase]).start()

        @pl.loop(1, n)
        def _(d):
            remote(src, dst, phase, d).start()

    def finish(src, dst, phase):
        @pl.loop(1, n)
        def _(d):
            arrival(src, dst, phase, d).wait_recv()

        pltpu.make_async_copy(src.at[me], dst.at[me], own_sem.at[phase]).wait()

    def drain(src, dst, phase):
        @pl.loop(1, n)
        def _(d):
            remote(src, dst, phase, d).wait_send()

    def forward(rows, spec):
        @pl.loop(0, n)
        def _(p):
            wide[pl.ds(pl.multiple_of(p * channels, 8), channels), :] = rows[p].astype(F32)

        @pl.loop(0, steps)
        def _(k):
            parts = []
            cos_t, sin_t = cos_ref[...], sin_ref[...]
            for i in range(group):
                x = wide[pl.ds(k * group + i, n, stride=channels), :].astype(BF16)
                z = dot(first_ref[...], x)
                z = z[: 2 * n] + z[2 * n :]
                re, im = z[:n], z[n:]
                parts.append(
                    jnp.concatenate([re * cos_t + im * sin_t, im * cos_t - re * sin_t], axis=1)
                )
            hi, lo = halves(jnp.concatenate(parts, axis=0))
            s = dot(hi, second_ref[0]) + dot(hi, second_ref[1]) + dot(lo, second_ref[0])
            spec[pl.ds(pl.multiple_of(k * group * n, 8), group * n), :] = s

    def inverse(left, right, conjugate):
        @pl.loop(0, steps)
        def _(k):
            here = pl.ds(pl.multiple_of(k * group * n, 8), group * n)
            a, b = left[here, :fine], left[here, fine:]
            c, d = right[here, :fine], right[here, fine:]
            if conjugate:
                s = jnp.concatenate([a * c + b * d, b * c - a * d], axis=1)
            else:
                s = jnp.concatenate([a * c - b * d, a * d + b * c], axis=1)
            hi, lo = halves(s)
            mid = dot(hi, back_ref[0]) + dot(hi, back_ref[1]) + dot(lo, back_ref[0])
            cos_t, sin_t = cos_ref[...], sin_ref[...]
            for i in range(group):
                re, im = mid[i * n : (i + 1) * n, :fine], mid[i * n : (i + 1) * n, fine:]
                t = jnp.concatenate([re * cos_t - im * sin_t, im * cos_t + re * sin_t], axis=0)
                hi_t, lo_t = halves(t)
                y = dot(last_ref[0], hi_t) + dot(last_ref[0], lo_t) + dot(last_ref[1], hi_t)
                result[pl.ds(k * group + i, n, stride=channels), :] = y

    def round_with_bias(rows, out):
        @pl.loop(0, n)
        def _(p):
            y = result[pl.ds(pl.multiple_of(p * channels, 8), channels), :]
            out[p] = (y + bias_ref[...] * rows[p].astype(F32)).astype(BF16)

    start(g_in, g_rows, 0)
    start(m_in, m_rows, 1)
    start(h_in, h_rows, 2)

    finish(g_in, g_rows, 0)
    forward(g_rows, g_spec)
    finish(m_in, m_rows, 1)
    forward(m_rows, m_spec)
    inverse(g_spec, m_spec, True)

    @pl.loop(0, n)
    def _(p):
        y = result[pl.ds(pl.multiple_of(p * channels, 8), channels), :]
        fg_send[p] = (y * scale).astype(BF16)

    start(fg_send, fg_out, 3)

    dot_out[...] = jnp.zeros_like(dot_out)

    @pl.loop(0, n)
    def _(p):
        dot_out[...] += g_rows[p].astype(F32) * m_rows[p].astype(F32)

    finish(h_in, h_rows, 2)
    forward(h_rows, h_spec)
    inverse(h_spec, m_spec, False)
    round_with_bias(m_rows, conv_send)
    start(conv_send, conv_out, 4)
    inverse(g_spec, h_spec, True)
    round_with_bias(g_rows, grad_send)
    start(grad_send, grad_out, 5)

    finish(fg_send, fg_out, 3)
    finish(conv_send, conv_out, 4)
    finish(grad_send, grad_out, 5)
    drain(g_in, g_rows, 0)
    drain(m_in, m_rows, 1)
    drain(h_in, h_rows, 2)
    drain(fg_send, fg_out, 3)
    drain(conv_send, conv_out, 4)
    drain(grad_send, grad_out, 5)


def make(n, inner_size):
    def on_device(query_gate, key_proj, value_proj, out_grad, filters, skip_bias):
        total_channels, fine = key_proj.shape
        channels = total_channels // n
        length = n * fine
        shape = (n, channels, fine)
        scale = 1.0 / math.sqrt(length)
        tabs = [jnp.asarray(t) for t in tables(n, fine)]

        gated = (out_grad.astype(F32) * query_gate.astype(F32)).astype(BF16).reshape(shape)
        mixed = (key_proj.astype(F32) * value_proj.astype(F32)).astype(BF16).reshape(shape)
        filt = filters.astype(BF16).reshape(shape)
        bias = jnp.broadcast_to(skip_bias[:, None], (channels, fine))

        vmem = pl.BlockSpec(memory_space=pltpu.VMEM)
        block = jax.ShapeDtypeStruct(shape, BF16)
        fg, conv, grad, dots = pl.pallas_call(
            functools.partial(kernel, n, inner_size, scale),
            out_shape=(block, block, block, jax.ShapeDtypeStruct((channels, fine), F32)),
            in_specs=[vmem] * 10,
            out_specs=(vmem,) * 4,
            scratch_shapes=[pltpu.VMEM(shape, BF16)] * 6
            + [pltpu.VMEM((total_channels, fine), F32)] * 2
            + [pltpu.VMEM((total_channels, 2 * fine), F32)] * 3
            + [
                pltpu.SemaphoreType.DMA((6, n)),
                pltpu.SemaphoreType.DMA((6, n)),
                pltpu.SemaphoreType.DMA((6,)),
            ],
            compiler_params=pltpu.CompilerParams(
                collective_id=0, has_side_effects=True, vmem_limit_bytes=60 * 1024 * 1024
            ),
        )(gated, mixed, filt, bias, *tabs)

        full = (total_channels, fine)
        conv_wide = conv.reshape(full).astype(F32)
        grad_wide = grad.reshape(full).astype(F32)
        output = (query_gate.astype(F32) * conv_wide).astype(BF16)
        query_grad = (out_grad.astype(F32) * conv_wide).astype(BF16)
        key_grad = (grad_wide * value_proj.astype(F32)).astype(BF16)
        value_grad = (grad_wide * key_proj.astype(F32)).astype(BF16)
        bias_grad = jnp.sum(dots, axis=1) * scale
        return (output, query_grad, key_grad, value_grad, fg.reshape(full).astype(F32), bias_grad)

    return on_device


def solution(mesh):
    n = math.prod(mesh.shape[a] for a in AXES)
    seq = P(None, AXES)
    return jax.shard_map(
        make(n, mesh.shape["inner"]),
        mesh=mesh,
        in_specs=(seq, seq, seq, seq, seq, P(AXES)),
        out_specs=(seq, seq, seq, seq, seq, P(AXES)),
        check_vma=False,
    )
```
